32 devices in a mesh: groups: 2 (over y), expert: 4 (over z), tensor: 4 (over x, core).
Axes of the slice: x: 2, y: 2, z: 4, core: 2. Of those that a mesh axis runs over, the one named last changes fastest.
Arguments:
- tokens: bfloat16 [256, 4096], P(('groups', 'expert'), 'tensor'), parts along dimension 0, may hold values from -6 to 6
- expert_ids: int32 [256, 8], P(('groups', 'expert')), parts along dimension 0, may hold values from 0 to 63, all different within a row; in each aligned block of 32 rows (0 to 31, 32 to 63, ...) at most 8 rows name the same one
- gate_fixed: int32 [256, 8], P(('groups', 'expert')), parts along dimension 0, may hold values from 1 to 65535
- w_gate: bfloat16 [64, 4096, 768], P('expert', None, 'tensor'), may hold values from -0.09375 to 0.09375
- w_up: bfloat16 [64, 4096, 768], P('expert', None, 'tensor'), may hold values from -0.09375 to 0.09375
- w_down: bfloat16 [64, 768, 4096], P('expert', 'tensor'), may hold values from -0.21875 to 0.21875
Outputs:
- mixed: bfloat16 [256, 4096], P(('groups', 'expert'), 'tensor'), parts along dimension 0
The draws below stay inside these ranges and needn't reach their ends.
There are 2 independent parts, one for each index of `groups`. The reference program is written for one: setup_inputs(seed, part) draws one part's arguments, and reference() takes and returns one part's arrays. A program takes and returns all parts, laid end to end along the dimension named above; an argument that names none is the same for every part. Nothing has to cross between parts.
Inputs may be any that keep to these rules, and one draw needn't show every extreme that they name: `expert_ids`: each row names 8 different experts. Within the 32 rows of one index of the expert axis no expert is named more than 8 times, and in every draw some expert is named exactly 8 times in some such block.
All inputs are finite; a program needn't handle non-finite values.
Results may differ from the reference program's by a relative error of at most 0.014.
Values may be sent and summed in bfloat16 or wider, within the bound.
A program may use at most 128 MiB of HBM per device.

```python
import math
import jax
import jax.numpy as jnp
import numpy as np
from jax import lax

D = 4096
FF = 768
EXPERTS = 64
TOP = 8
TOK_DEV = 32
CAP = 8
TOKENS = 128
N_TENSOR = 4


def plant(result, rng, smallest, top_value):
    longest = result.shape.index(max(result.shape))
    spots = []
    for shift in (0, 1):
        where = [jax.random.randint(jax.random.fold_in(rng, axis), (), 0, length) for axis, length in enumerate(result.shape)]
        where[longest] = (where[longest] + shift) % result.shape[longest]
        spots.append(tuple(where))
    return result.at[spots[0]].set(smallest).at[spots[1]].set(top_value)


def block_scale(rng, extent, shards, least, top_value):
    factor_of, own = 1.0, jax.random.fold_in(rng, 6)
    for axis_at, parts in shards:
        steps = jnp.exp(jax.random.uniform(jax.random.fold_in(own, axis_at), (parts,), jnp.float32, least / len(shards), top_value / len(shards)))
        factor_of = factor_of * jnp.repeat(steps, extent[axis_at] // parts).reshape([-1 if axis == axis_at else 1 for axis in range(len(extent))])
    return factor_of


def deal_out(rng, own, number, rows, number_of, top, most, lean):
    order = jax.random.permutation(rng, number_of)
    crowded, usual = portions_of(number_of, rows * top, most, lean, True), portions_of(number_of, rows * top, most, lean, False)
    places = jnp.arange(number_of)

    def named(sizes, rotation):
        used = int((sizes > 0).sum())
        fixed = max(1, used // 4)
        shifted = fixed + (places - fixed + rotation * (used - fixed)) % max(1, number_of - fixed)
        return jnp.zeros((number_of,), jnp.int32).at[order[jnp.where(places < fixed, places, shifted)]].set(jnp.asarray(sizes, jnp.int32))

    sizes = jnp.where(number % 4 == 0, named(crowded, number // 4), named(usual, number - number // 4 - 1))
    mixed = jax.random.permutation(jax.random.fold_in(own, 3), number_of)
    source_of, sink = mixed[0:number_of // 2 * 2:2], mixed[1:number_of // 2 * 2:2]
    slack = jnp.minimum(sizes[source_of] - 1, most - sizes[sink]) // 2
    slack = jnp.where((source_of == order[0]) | (sink == order[0]) | (sizes[sink] == 0), 0, jnp.maximum(slack, 0))
    shifted = jax.random.randint(jax.random.fold_in(own, 4), (number_of // 2,), 0, 1 << 20) % (slack + 1)
    sizes = sizes.at[source_of].add(-shifted).at[sink].add(shifted)
    items = jnp.searchsorted(jnp.cumsum(sizes), jnp.arange(rows * top), side="right").astype(jnp.int32)
    table = items.reshape(top, rows).T
    table = table[jax.random.permutation(jax.random.fold_in(own, 1), rows)]
    rotation = jax.random.randint(jax.random.fold_in(own, 2), (rows, 1), 0, top)
    return jnp.take_along_axis(table, (jnp.arange(top)[None, :] + rotation) % top, axis=1)


def portions_of(amount, total, reach, skew, full):
    loads = [(1 << 20) // math.isqrt(rank ** skew) + 1 for rank in range(1, amount + 1)]
    largest = reach if full else min(reach, max(-(-total // amount), total * loads[0] // sum(loads)))
    least = 1 if total - largest >= amount - 1 else 0
    counts, rest = [largest] + [least] * (amount - 1), total - largest - least * (amount - 1)
    while rest > 0:
        free = [i for i in range(1, amount) if counts[i] < largest] or [i for i in range(1, amount) if counts[i] < reach]
        pool, left = sum([loads[i] for i in free]), rest
        for i in free:
            extra = min(reach - counts[i], max(1, left * loads[i] // pool), rest)
            counts[i] = counts[i] + extra
            rest = rest - extra
    return np.array(counts)


def gaussian(stream_key, extent, width, bound, pieces=(), kind=jnp.bfloat16):
    level = block_scale(stream_key, extent, pieces, -0.22, 0.18) if pieces else 1.0
    entries = jax.random.normal(stream_key, extent, jnp.float32) * width * level
    return jnp.minimum(jnp.maximum(entries, -bound), bound).astype(kind)


def setup_inputs(seed: int = 0, part: int = 0) -> dict:
    key_list = jax.random.split(jax.random.key(seed), 7)
    part_splits = jax.random.split(jax.random.fold_in(key_list[6], part), 7)
    tokens = gaussian(part_splits[0], (TOKENS, D), 1.0, 6.0, ((0, 4), (1, 4)))
    expert_ids_keys = jax.random.split(jax.random.fold_in(part_splits[1], 1), TOKENS // TOK_DEV)
    expert_ids_turns = jax.random.permutation(jax.random.fold_in(part_splits[1], 3), TOKENS // TOK_DEV)
    expert_ids = jax.vmap(lambda own, number: deal_out(jax.random.fold_in(part_splits[1], 2), own, number, TOK_DEV, EXPERTS, TOP, CAP, 2))(expert_ids_keys, expert_ids_turns).reshape((TOKENS, TOP))
    gate_fixed = plant(jax.random.randint(part_splits[2], (TOKENS, TOP), 1, 65536), jax.random.fold_in(part_splits[2], 1), 1, 65535).astype(jnp.int32)
    w_gate = gaussian(key_list[3], (EXPERTS, D, FF), D ** -0.5, 0.09375, ((0, 4), (2, 4)))
    w_up = gaussian(key_list[4], (EXPERTS, D, FF), D ** -0.5, 0.09375, ((0, 4), (2, 4)))
    w_down = gaussian(key_list[5], (EXPERTS, FF, D), FF ** -0.5, 0.21875, ((0, 4), (1, 4)))
    return dict(tokens=tokens, expert_ids=expert_ids, gate_fixed=gate_fixed, w_gate=w_gate, w_up=w_up, w_down=w_down)


def reference(tokens, expert_ids, gate_fixed, w_gate, w_up, w_down):
    weights = gate_fixed.astype(jnp.float32)
    gate_share = weights / jnp.sum(weights, axis=1, keepdims=True)
    group_width = FF // N_TENSOR

    def one_expert(running, expert_index):
        chosen = jnp.sum(jnp.where(expert_ids == expert_index, gate_share, jnp.zeros_like(gate_share)), axis=1)
        gate_proj = jnp.dot(tokens, w_gate[expert_index], preferred_element_type=jnp.float32)
        up_proj = jnp.dot(tokens, w_up[expert_index], preferred_element_type=jnp.float32)
        hidden = (jax.nn.silu(gate_proj) * up_proj).astype(jnp.bfloat16)
        down = w_down[expert_index]
        summed = jnp.zeros((tokens.shape[0], D), jnp.float32)
        for piece_index in range(N_TENSOR):
            lower = piece_index * group_width
            group_term = jnp.dot(hidden[:, lower:lower + group_width], down[lower:lower + group_width], preferred_element_type=jnp.float32)
            summed = summed + lax.optimization_barrier(group_term.astype(jnp.bfloat16)).astype(jnp.float32)
        expert_out = lax.optimization_barrier(summed.astype(jnp.bfloat16)).astype(jnp.float32)
        return running + chosen[:, None] * expert_out, None

    start = jnp.zeros((tokens.shape[0], D), jnp.float32)
    running, unused = lax.scan(one_expert, start, jnp.arange(EXPERTS, dtype=jnp.int32))
    return running.astype(jnp.bfloat16)
```

```python
import functools

import jax
import jax.numpy as jnp
from jax import lax
from jax.experimental import pallas as pl
from jax.experimental.pallas import tpu as pltpu
from jax.sharding import PartitionSpec as P

CAP = 8


def expert_block(slot_rows, w_gate, w_up, w_down):
    gate_proj = jnp.einsum("gekd,edf->gekf", slot_rows, w_gate, preferred_element_type=jnp.float32)
    up_proj = jnp.einsum("gekd,edf->gekf", slot_rows, w_up, preferred_element_type=jnp.float32)
    hidden = (jax.nn.silu(gate_proj) * up_proj).astype(jnp.bfloat16)
    partial_value = jnp.einsum("gekf,efd->gekd", hidden, w_down, preferred_element_type=jnp.float32)
    summed = lax.psum_scatter(
        partial_value.astype(jnp.bfloat16), "tensor", scatter_dimension=3, tiled=True
    )
    return lax.all_to_all(summed, "expert", split_axis=0, concat_axis=0, tiled=True)


def slotted(tokens, expert_ids, gate_fixed, w_gate, w_up, w_down):
    tok_rows, per_token = expert_ids.shape
    local_experts = w_gate.shape[0]
    devices_e = lax.axis_size("expert")
    experts = local_experts * devices_e
    capacity = CAP
    flat_ids = expert_ids.reshape(-1)
    pick_count = tok_rows * per_token
    onehot = (flat_ids[:, None] == jnp.arange(experts, dtype=jnp.int32)[None, :]).astype(jnp.int32)
    before = jnp.cumsum(onehot, axis=0) - onehot
    slot_rank = jnp.sum(before * onehot, axis=1)
    slot_index = flat_ids * capacity + slot_rank
    owner_row = jnp.arange(pick_count, dtype=jnp.int32) // per_token
    slot_token = jnp.full((experts * capacity,), tok_rows, jnp.int32).at[slot_index].set(owner_row)
    padded = jnp.concatenate([tokens, jnp.zeros((1, tokens.shape[1]), tokens.dtype)], axis=0)
    returned = expert_block(
        lax.all_gather(
            lax.all_to_all(
                padded[slot_token].reshape(devices_e, local_experts, capacity, tokens.shape[1]),
                "expert",
                split_axis=0,
                concat_axis=0,
                tiled=True,
            ),
            "tensor",
            axis=3,
            tiled=True,
        ),
        w_gate,
        w_up,
        w_down,
    )
    flat_returned = returned.reshape(experts * capacity, returned.shape[3])
    picked = flat_returned[slot_index].reshape(tok_rows, per_token, returned.shape[3])
    weights = gate_fixed.astype(jnp.float32)
    gate_share = weights / jnp.sum(weights, axis=1, keepdims=True)
    mixed_out = jnp.einsum("tk,tkf->tf", gate_share, picked.astype(jnp.float32))
    return mixed_out.astype(jnp.bfloat16)


MESH = pl.DeviceIdType.MESH
VMEM_BYTES = 67_000_000
LANES = 128
TILE = 256
SUMS = 6
PRE = 18


def fused_kernel(*args):
    def body(*sums):
        fused_body(sums[:SUMS], sums[SUMS:], *args)

    shape = (args[0] * args[4], TILE)
    pl.run_scoped(body, *[pltpu.ACC(q)(shape, jnp.float32) for q in range(2) for _ in range(SUMS)])


def fused_body(
    sums0, sums1, tok_rows, feats, experts, hidden_units, E, T,
    x_ref, ids_ref, gates_ref, wg_ref, wu_ref, wd_ref, out_ref,
    pool, tok, ids_all, gates_all, acc, hid,
    to_partner, from_partner, to_x, from_x, to_z, from_z, own,
    w_sem, own_sem, zt_send, zt_recv, zi_send, zi_recv, t_send, t_recv,
    p_send, p_recv, x_send, x_recv, z_send, z_recv,
):
    g, e, t = lax.axis_index("groups"), lax.axis_index("expert"), lax.axis_index("tensor")
    X = T // 2
    x, c = lax.div(t, 2), lax.rem(t, 2)
    pairs, half = experts // 2, experts // 4
    wide = 2 * hidden_units
    tall = 2 * wide

    def peer(k):
        half_k, side = k // 2, k % 2
        return lax.rem(x + half_k, X) * 2 + lax.rem(c + side, 2)

    def mirror(k):
        return (-(k // 2)) % X * 2 + k % 2

    def rows_of(block):
        return pl.ds(pl.multiple_of(block * tok_rows, tok_rows), tok_rows)

    def features_of(k):
        return pl.ds(pl.multiple_of(peer(k) * feats, feats), feats)

    def fetch(k, p):
        slot = k * pairs + p
        for part, w in enumerate((wg_ref, wu_ref)):
            for j in range(2):
                pltpu.make_async_copy(
                    w.at[2 * p + j, :, features_of(k)],
                    pool.at[slot, pl.ds(part * wide + j * hidden_units, hidden_units), :],
                    w_sem.at[slot],
                ).start()

    def fetched(slot):
        pltpu.make_async_copy(pool.at[slot], pool.at[slot], w_sem.at[slot]).wait()

    down_slot = {T - 1: T * pairs, T - 2: 0, 1: pairs, 0: half}

    def fetch_down(k):
        for q in range(half):
            slot = down_slot[k] + q
            pltpu.make_async_copy(
                wd_ref.at[pl.ds(q * tall, tall), features_of(k)], pool.at[slot], w_sem.at[slot]
            ).start()

    def turn_band(slot, r):
        at = (slot, slice(r * LANES, (r + 1) * LANES))
        band = pool[at]
        pool[at] = jnp.concatenate(
            [jnp.transpose(band[:, f * LANES:(f + 1) * LANES]) for f in range(feats // LANES)], axis=1
        )

    def turn(slot):
        for r in range(tall // LANES):
            turn_band(slot, r)

    def turned(slot, n, f):
        bands = [
            pool[slot, (2 * n + r) * LANES:(2 * n + r + 1) * LANES, f * TILE:(f + 1) * TILE] for r in range(2)
        ]
        return jnp.concatenate(
            [jnp.concatenate([band[:, j * LANES:(j + 1) * LANES] for band in bands], axis=1) for j in range(2)],
            axis=0,
        )

    sums, stage, turn_of = (sums0, sums1), [0, 0], [0, 0]

    def multiply(jobs, lag, side=()):
        side, done, total = list(side), 0, sum(len(steps) for steps, _ in jobs[0])
        begun = len(side)
        waiting = []
        for pair in zip(*jobs):
            used = []
            for q in range(2):
                used.append(sums[q][turn_of[q] % SUMS])
                turn_of[q] += 1
            for s in range(len(pair[0][0])):
                for q in range(2):
                    rows, weights, flip = pair[q][0][s]
                    at = stage[q] % 2
                    stage[q] += 1
                    pltpu.matmul_push_rhs(weights(), staging_register=at, mxu_index=q, transpose=flip)
                    pltpu.matmul_acc_lhs(used[q], rows(), load_staged_rhs=at)
                done += 1
                while side and begun - len(side) < begun * done // total:
                    side.pop(0)()
            waiting.append([(pair[q][1], used[q]) for q in range(2)])
            while len(waiting) > lag:
                for sink, used_sum in waiting.pop(0):
                    sink(pltpu.matmul_pop(used_sum))
        for rest in waiting:
            for sink, used_sum in rest:
                sink(pltpu.matmul_pop(used_sum))

    local = [
        pltpu.make_async_copy(x_ref, tok.at[0, rows_of(e), :], own_sem.at[0]),
        pltpu.make_async_copy(ids_ref, ids_all.at[e], own_sem.at[1]),
        pltpu.make_async_copy(gates_ref, gates_all.at[e], own_sem.at[2]),
    ]
    for copy in local:
        copy.start()
    for k in range(2):
        @pl.loop(0, pairs)
        def _(p, k=k):
            fetch(k, p)

    barrier = pltpu.get_barrier_semaphore()
    for d in range(1, E):
        pl.semaphore_signal(barrier, inc=1, device_id=(g, lax.rem(e + d, E), t), device_id_type=MESH)
    for k in range(1, T):
        pl.semaphore_signal(barrier, inc=1, device_id=(g, e, peer(k)), device_id_type=MESH)

    def turn_range(first, last):
        @pl.loop(first, last)
        def _(slot):
            fetched(slot)
            turn(slot)

    turn_range(0, 2)
    pl.semaphore_wait(barrier, E - 1 + T - 1)

    def remote(src, dst, send, recv, where):
        return pltpu.make_async_remote_copy(
            src_ref=src, dst_ref=dst, send_sem=send, recv_sem=recv, device_id=where, device_id_type=MESH
        )

    for copy in local:
        copy.wait()
    held = tok.at[0, rows_of(e), :]
    sent = []

    def go(*args):
        copy = remote(*args)
        copy.start()
        sent.append(copy)

    def arrived(dst, send, recv):
        remote(dst, dst, send, recv, (g, e, peer(1))).wait_recv()

    def spread(source, d):
        block = lax.rem(e + E - d, E)
        for k in [1] + [2 * dx for dx in range(1, X)]:
            m = mirror(k)
            go(source, tok.at[m, rows_of(block), :], t_send.at[k, d], t_recv.at[m, d], (g, e, peer(k)))

    for d in range(1, E):
        where = (g, lax.rem(e + d, E), t)
        go(held, held, zt_send.at[d], zt_recv.at[d], where)
    spread(held, 0)
    for d in range(1, E):
        where = (g, lax.rem(e + d, E), t)
        go(ids_all.at[e], ids_all.at[e], zi_send.at[0, d], zi_recv.at[0, d], where)
        go(gates_all.at[e], gates_all.at[e], zi_send.at[1, d], zi_recv.at[1, d], where)
    for k in range(2, T):
        @pl.loop(0, pairs)
        def _(p, k=k):
            fetch(k, p)
    fetch_down(T - 1)

    def from_side(k, d):
        landed = tok.at[k, rows_of(lax.rem(e + E - d, E)), :]
        arrived(landed, t_send.at[k, d], t_recv.at[k, d])
        return landed

    def pass_on(d):
        for k in range(2, T, 2):
            block = lax.rem(e + E - d, E)
            go(
                from_side(k, d), tok.at[k + 1, rows_of(block), :],
                t_send.at[k + 1, d], t_recv.at[k + 1, d], (g, e, peer(1)),
            )

    marks = [2] + [PRE - 7 + (PRE - PRE + 7) * (d - 1) // (E - 1) for d in range(1, E)] + [PRE]
    for d in range(1, E):
        turn_range(marks[d - 1], marks[d])
        landed = tok.at[0, rows_of(lax.rem(e + E - d, E)), :]
        arrived(landed, zt_send.at[d], zt_recv.at[d])
        spread(landed, d)
    turn_range(marks[E - 1], PRE)
    for d in range(E):
        from_side(1, d)

    def early(first, last):
        for slot in range(first, last):
            fetched(slot)
        return range(first, last)

    def steps_of(p, n, ks, flip):
        def step(k, f):
            slot = k * pairs + p
            return (
                lambda: tok[k, :, f * TILE:(f + 1) * TILE],
                lambda: pool[slot, n * TILE:(n + 1) * TILE, f * TILE:(f + 1) * TILE] if flip else turned(slot, n, f),
                flip,
            )

        return [step(k, f) for k in ks for f in range(feats // TILE)]

    tiles = tall // TILE

    def sink_of(p, n, first, last):
        def sink(value):
            at = (p, slice(None), slice(n * TILE, (n + 1) * TILE))
            acc[at] = value if first else acc[at] + value
            if last and n == tiles - 1:
                finish(p)

        return sink

    def jobs_of(members, ks, first=False, last=False, flip=False):
        return [
            [
                (steps_of(p, n, ks, flip), sink_of(p, n, first, last))
                for p in members[q::2] for n in range(tiles)
            ]
            for q in range(2)
        ]

    def bands_of(slots):
        return [functools.partial(turn_band, slot, r) for slot in slots for r in range(tall // LANES)]

    low, high = list(range(half)), list(range(half, pairs))
    third, fourth = 2 * pairs, 3 * pairs
    pass_on(0)
    multiply(jobs_of(low, (0, 1), first=True), 1, bands_of(early(PRE, third + half)))
    fetch_down(T - 2)
    fetch_down(1)
    for d in range(1, E):
        pass_on(d)
    multiply(jobs_of(high, (0, 1), first=True), 1, bands_of(early(third + half, fourth)))
    fetch_down(0)
    for d in range(E):
        from_side(T - 1, d)
    for d in range(1, E):
        s = lax.rem(e + E - d, E)
        arrived(ids_all.at[s], zi_send.at[0, d], zi_recv.at[0, d])
        arrived(gates_all.at[s], zi_send.at[1, d], zi_recv.at[1, d])
    ids = jnp.concatenate([ids_all[s] for s in range(E)], axis=1)
    gates = jnp.concatenate([gates_all[s] for s in range(E)], axis=1).astype(jnp.float32)
    share = jnp.transpose(gates / jnp.sum(gates, axis=0, keepdims=True))
    ids = jnp.transpose(ids)
    first_of_pair = lax.broadcasted_iota(jnp.int32, (E * tok_rows, wide), 1) < hidden_units

    def finish(p):
        both = acc[p]
        gate, up = both[:, :wide], both[:, wide:]
        weight = [
            jnp.sum(jnp.where(ids == e * experts + 2 * p + j, share, 0.0), axis=1, keepdims=True)
            for j in range(2)
        ]
        value = gate / (1.0 + jnp.exp(-gate)) * up * jnp.where(first_of_pair, weight[0], weight[1])
        hid[:, p * wide:(p + 1) * wide] = value.astype(jnp.bfloat16)

    multiply(jobs_of(low + high, (2,)), 1, bands_of(early(fourth, fourth + half)))
    late = high[half // 2:]
    some = early(fourth + half, fourth + half + half // 2)
    for p in late:
        fetched(fourth + p)
    plain, flipped = jobs_of(low, (3,), last=True), jobs_of(late, (3,), last=True, flip=True)
    multiply([plain[q] + flipped[q] for q in range(2)], 1, bands_of(some))
    multiply(jobs_of(high[:half // 2], (3,), last=True), 1)

    parts_n = feats // TILE
    def down_jobs(k, n, sinks):
        if n == 0:
            for q in range(half):
                fetched(down_slot[k] + q)

        def step(q, m, f):
            start = m * tall + f * TILE
            return (
                lambda: hid[:, start:start + TILE],
                lambda: pool[
                    down_slot[k] + m, f * TILE:(f + 1) * TILE, (n + q) * TILE:(n + q + 1) * TILE
                ],
                False,
            )

        multiply(
            [[([step(q, m, f) for m in range(half) for f in range(tiles)], sinks(n + q))] for q in range(2)], 0
        )

    def to_side(dx, n):
        def sinks(n):
            def sink(value):
                to_partner[dx, n] = value.astype(jnp.bfloat16)
                go(
                    to_partner.at[dx, n], from_partner.at[dx, n],
                    p_send.at[dx, n], p_recv.at[dx, n], (g, e, peer(1)),
                )

            return sink

        down_jobs(2 * dx + 1, n, sinks)

    def meet_side(dx, n):
        def sinks(n):
            def sink(value):
                arrived(from_partner.at[dx, n], p_send.at[dx, n], p_recv.at[dx, n])
                met = value + from_partner[dx, n].astype(jnp.float32)
                if dx:
                    back = (X - dx) % X
                    to_x[dx, n] = met.astype(jnp.bfloat16)
                    go(
                        to_x.at[dx, n], from_x.at[back, n],
                        x_send.at[dx, n], x_recv.at[back, n], (g, e, peer(2 * dx)),
                    )
                else:
                    own[n] = met

            return sink

        down_jobs(2 * dx, n, sinks)

    for dx in reversed(range(X)):
        for n in range(0, parts_n, 2):
            to_side(dx, n)
        for n in range(0, parts_n, 2):
            meet_side(dx, n)
    for n in range(parts_n):
        for other in range(1, X):
            arrived(from_x.at[other, n], x_send.at[other, n], x_recv.at[other, n])
            own[n] += from_x[other, n].astype(jnp.float32)
        for j in range(1, E):
            to_z[j, n] = own[n, rows_of(lax.rem(e + j, E)), :].astype(jnp.bfloat16)
            go(to_z.at[j, n], from_z.at[j, n], z_send.at[j, n], z_recv.at[j, n], (g, lax.rem(e + j, E), t))
    for n in range(parts_n):
        total = own[n, rows_of(e), :]
        for d in range(1, E):
            arrived(from_z.at[d, n], z_send.at[d, n], z_recv.at[d, n])
            total += from_z[d, n].astype(jnp.float32)
        out_ref[:, n * TILE:(n + 1) * TILE] = total.astype(out_ref.dtype)
    for copy in sent:
        copy.wait_send()


def scratch_of(tok_rows, feats, experts, hidden_units, E, T, per_token):
    bf16, f32, X, N = jnp.bfloat16, jnp.float32, T // 2, E * tok_rows
    parts_n, tall = feats // TILE, 4 * hidden_units
    slots = T * experts // 2 + experts // 4
    dma = pltpu.SemaphoreType.DMA
    return [
        ((slots, tall, feats), bf16),
        ((T, N, feats), bf16),
        ((E, per_token, tok_rows), jnp.int32),
        ((E, per_token, tok_rows), jnp.int32),
        ((experts // 2, N, tall), f32),
        ((N, experts * hidden_units), bf16),
        ((X, parts_n, N, TILE), bf16),
        ((X, parts_n, N, TILE), bf16),
        ((X, parts_n, N, TILE), bf16),
        ((X, parts_n, N, TILE), bf16),
        ((E, parts_n, tok_rows, TILE), bf16),
        ((E, parts_n, tok_rows, TILE), bf16),
        ((parts_n, N, TILE), f32),
    ], [
        dma((slots,)), dma((3,)),
        dma((E,)), dma((E,)), dma((2, E)), dma((2, E)), dma((T, E)), dma((T, E)),
        dma((X, parts_n)), dma((X, parts_n)), dma((X, parts_n)), dma((X, parts_n)), dma((E, parts_n)), dma((E, parts_n)),
    ]


def fits_fused(sizes):
    tok_rows, feats, experts, hidden_units, E, T, per_token = sizes
    if T != 4 or E < 2 or experts != 16 or E * tok_rows != 128 or feats % 512 or tok_rows % 16:
        return False
    if 2 * hidden_units % 128 or hidden_units % 16:
        return False
    buffers, _ = scratch_of(*sizes)
    size = 0
    for shape, kind in buffers:
        count = jnp.dtype(kind).itemsize
        for length in shape:
            count *= length
        size += count
    return size < VMEM_BYTES - 1_000_000


def on_device(tokens, expert_ids, gate_fixed, w_gate, w_up, w_down):
    (tok_rows, feats), per_token = tokens.shape, expert_ids.shape[1]
    experts, width, hidden_units = w_gate.shape
    E, T = lax.axis_size("expert"), lax.axis_size("tensor")
    sizes = (tok_rows, feats, experts, hidden_units, E, T, per_token)
    if not fits_fused(sizes):
        return slotted(tokens, expert_ids, gate_fixed, w_gate, w_up, w_down)
    buffers, semaphores = scratch_of(*sizes)
    vmem, anywhere = pl.BlockSpec(memory_space=pltpu.VMEM), pl.BlockSpec(memory_space=pl.ANY)
    return pl.pallas_call(
        functools.partial(fused_kernel, *sizes[:6]),
        out_shape=jax.ShapeDtypeStruct(tokens.shape, tokens.dtype),
        in_specs=[anywhere] * 6,
        out_specs=vmem,
        scratch_shapes=[pltpu.VMEM(shape, kind) for shape, kind in buffers] + semaphores,
        compiler_params=pltpu.CompilerParams(
            collective_id=0, has_side_effects=True, vmem_limit_bytes=VMEM_BYTES
        ),
    )(
        tokens,
        expert_ids.T,
        gate_fixed.T,
        jnp.swapaxes(w_gate, 1, 2),
        jnp.swapaxes(w_up, 1, 2),
        w_down.reshape(experts * hidden_units, width),
    )


def solution(mesh):
    placed = (
        P(("groups", "expert"), "tensor"),
        P(("groups", "expert"), None),
        P(("groups", "expert"), None),
        P("expert", None, "tensor"),
        P("expert", None, "tensor"),
        P("expert", "tensor", None),
    )
    return jax.shard_map(
        on_device,
        mesh=mesh,
        in_specs=placed,
        out_specs=P(("groups", "expert"), "tensor"),
        check_vma=False,
    )
```

```python
import functools

import jax
import jax.numpy as jnp
from jax import lax
from jax.experimental import pallas as pl
from jax.experimental.pallas import tpu as pltpu
from jax.sharding import PartitionSpec as P

CAP = 8


def expert_block(slot_rows, w_gate, w_up, w_down):
    gate_proj = jnp.einsum("gekd,edf->gekf", slot_rows, w_gate, preferred_element_type=jnp.float32)
    up_proj = jnp.einsum("gekd,edf->gekf", slot_rows, w_up, preferred_element_type=jnp.float32)
    hidden = (jax.nn.silu(gate_proj) * up_proj).astype(jnp.bfloat16)
    partial_value = jnp.einsum("gekf,efd->gekd", hidden, w_down, preferred_element_type=jnp.float32)
    summed = lax.psum_scatter(
        partial_value.astype(jnp.bfloat16), "tensor", scatter_dimension=3, tiled=True
    )
    return lax.all_to_all(summed, "expert", split_axis=0, concat_axis=0, tiled=True)


def slotted(tokens, expert_ids, gate_fixed, w_gate, w_up, w_down):
    tok_rows, per_token = expert_ids.shape
    local_experts = w_gate.shape[0]
    devices_e = lax.axis_size("expert")
    experts = local_experts * devices_e
    capacity = CAP
    flat_ids = expert_ids.reshape(-1)
    pick_count = tok_rows * per_token
    onehot = (flat_ids[:, None] == jnp.arange(experts, dtype=jnp.int32)[None, :]).astype(jnp.int32)
    before = jnp.cumsum(onehot, axis=0) - onehot
    slot_rank = jnp.sum(before * onehot, axis=1)
    slot_index = flat_ids * capacity + slot_rank
    owner_row = jnp.arange(pick_count, dtype=jnp.int32) // per_token
    slot_token = jnp.full((experts * capacity,), tok_rows, jnp.int32).at[slot_index].set(owner_row)
    padded = jnp.concatenate([tokens, jnp.zeros((1, tokens.shape[1]), tokens.dtype)], axis=0)
    returned = expert_block(
        lax.all_gather(
            lax.all_to_all(
                padded[slot_token].reshape(devices_e, local_experts, capacity, tokens.shape[1]),
                "expert",
                split_axis=0,
                concat_axis=0,
                tiled=True,
            ),
            "tensor",
            axis=3,
            tiled=True,
        ),
        w_gate,
        w_up,
        w_down,
    )
    flat_returned = returned.reshape(experts * capacity, returned.shape[3])
    picked = flat_returned[slot_index].reshape(tok_rows, per_token, returned.shape[3])
    weights = gate_fixed.astype(jnp.float32)
    gate_share = weights / jnp.sum(weights, axis=1, keepdims=True)
    mixed_out = jnp.einsum("tk,tkf->tf", gate_share, picked.astype(jnp.float32))
    return mixed_out.astype(jnp.bfloat16)


MESH = pl.DeviceIdType.MESH
VMEM_BYTES = 66_500_000
LANES = 128
TILE = 256
SUMS = 6
LAG = 1
PRE = 16


def fused_kernel(*args):
    tok_rows, feats, experts, _, E, T = args[:6]
    shape, parts_n, dma = (tok_rows * E, TILE), feats // TILE, pltpu.SemaphoreType.DMA

    def body(*scoped):
        fused_body(scoped[:SUMS], scoped[SUMS:2 * SUMS], scoped[2 * SUMS:], *args)

    pl.run_scoped(
        body, *[pltpu.ACC(q)(shape, jnp.float32) for q in range(2) for _ in range(SUMS)],
        dma((slots_of(experts, T),)), dma((3,)), dma((E,)), dma((2, E)), dma((T, E)),
        dma((T // 2, parts_n)), dma((T // 2, parts_n)), dma((E, parts_n)),
    )


def slots_of(experts, T):
    return T * experts // 2 + experts // 4


def fused_body(
    sums0, sums1, local_sems, tok_rows, feats, experts, hidden_units, E, T,
    x_ref, ids_ref, gates_ref, wg_ref, wu_ref, wd_ref, out_ref,
    pool, tok, ids_all, gates_all, acc, hid,
    to_partner, from_partner, to_x, from_x, to_z, from_z, own,
    zt_recv, zi_recv, t_recv, p_recv, x_recv, z_recv,
):
    w_sem, own_sem, zt_send, zi_send, t_send, p_send, x_send, z_send = local_sems
    g, e, t = lax.axis_index("groups"), lax.axis_index("expert"), lax.axis_index("tensor")
    X = T // 2
    x, c = lax.div(t, 2), lax.rem(t, 2)
    pairs, half = experts // 2, experts // 4
    wide = 2 * hidden_units
    tall = 2 * wide

    def peer(k):
        half_k, side = k // 2, k % 2
        return lax.rem(x + half_k, X) * 2 + lax.rem(c + side, 2)

    def mirror(k):
        return (-(k // 2)) % X * 2 + k % 2

    def rows_of(block):
        return pl.ds(pl.multiple_of(block * tok_rows, tok_rows), tok_rows)

    def features_of(k):
        return pl.ds(pl.multiple_of(peer(k) * feats, feats), feats)

    def fetch(k, p):
        slot = k * pairs + p
        for part, w in enumerate((wg_ref, wu_ref)):
            for j in range(2):
                pltpu.make_async_copy(
                    w.at[2 * p + j, :, features_of(k)],
                    pool.at[slot, pl.ds(part * wide + j * hidden_units, hidden_units), :],
                    w_sem.at[slot],
                ).start()

    def fetched(slot):
        pltpu.make_async_copy(pool.at[slot], pool.at[slot], w_sem.at[slot]).wait()

    down_slot = {T - 1: T * pairs, T - 2: 0, 1: pairs, 0: half}

    def fetch_down(k):
        for q in range(half):
            slot = down_slot[k] + q
            pltpu.make_async_copy(
                wd_ref.at[pl.ds(q * tall, tall), features_of(k)], pool.at[slot], w_sem.at[slot]
            ).start()

    def turn_band(slot, r):
        at = (slot, slice(r * LANES, (r + 1) * LANES))
        band = pool[at]
        pool[at] = jnp.concatenate(
            [jnp.transpose(band[:, f * LANES:(f + 1) * LANES]) for f in range(feats // LANES)], axis=1
        )

    def turn(slot):
        for r in range(tall // LANES):
            turn_band(slot, r)

    def turned(slot, n, f):
        bands = [
            pool[slot, (2 * n + r) * LANES:(2 * n + r + 1) * LANES, f * TILE:(f + 1) * TILE] for r in range(2)
        ]
        return jnp.concatenate(
            [jnp.concatenate([band[:, j * LANES:(j + 1) * LANES] for band in bands], axis=1) for j in range(2)],
            axis=0,
        )

    sums, stage, turn_of = (sums0, sums1), [0, 0], [0, 0]

    def multiply(jobs, lag, side=(), pause=None):
        side, done = list(side), 0
        total, begun = sum(len(steps) for steps, _ in jobs[0]), len(side)
        waiting = []

        def run(pair, used, steps):
            nonlocal done
            for s in steps:
                for q in range(2):
                    rows, weights, flip = pair[q][0][s]
                    at = stage[q] % 2
                    stage[q] += 1
                    pltpu.matmul_push_rhs(weights(), staging_register=at, mxu_index=q, transpose=flip)
                    pltpu.matmul_acc_lhs(used[q], rows(), load_staged_rhs=at)
                done += 1
                while side and begun - len(side) < begun * done // total:
                    side.pop(0)()

        def drain(limit):
            while len(waiting) > limit:
                for sink, used_sum in waiting.pop(0):
                    sink(pltpu.matmul_pop(used_sum))

        pairs_of = list(zip(*jobs))
        uses = []
        for _ in pairs_of:
            uses.append([sums[q][turn_of[q] % SUMS] for q in range(2)])
            for q in range(2):
                turn_of[q] += 1
        cut = 0
        if pause is not None:
            cut = len(jobs[0][0][0]) // 2
            for pair, used in zip(pairs_of, uses):
                run(pair, used, range(cut))
            pause()
        for pair, used in zip(pairs_of, uses):
            run(pair, used, range(cut, len(pair[0][0])))
            waiting.append([(pair[q][1], used[q]) for q in range(2)])
            drain(lag)
        drain(0)

    local = [
        pltpu.make_async_copy(x_ref, tok.at[0, rows_of(e), :], own_sem.at[0]),
        pltpu.make_async_copy(ids_ref, ids_all.at[e], own_sem.at[1]),
        pltpu.make_async_copy(gates_ref, gates_all.at[e], own_sem.at[2]),
    ]
    for copy in local:
        copy.start()
    for k in range(2):
        @pl.loop(0, pairs)
        def _(p, k=k):
            fetch(k, p)

    barrier = pltpu.get_barrier_semaphore()
    for d in range(1, E):
        pl.semaphore_signal(barrier, inc=1, device_id=(g, lax.rem(e + d, E), t), device_id_type=MESH)
    for k in range(1, T):
        pl.semaphore_signal(barrier, inc=1, device_id=(g, e, peer(k)), device_id_type=MESH)

    def turn_range(first, last):
        @pl.loop(first, last)
        def _(slot):
            fetched(slot)
            turn(slot)

    turn_range(0, 2)
    pl.semaphore_wait(barrier, E - 1 + T - 1)

    def remote(src, dst, send, recv, where):
        return pltpu.make_async_remote_copy(
            src_ref=src, dst_ref=dst, send_sem=send, recv_sem=recv, device_id=where, device_id_type=MESH
        )

    for copy in local:
        copy.wait()
    held = tok.at[0, rows_of(e), :]
    sent = []

    def go(*args):
        copy = remote(*args)
        copy.start()
        sent.append(copy)

    def arrived(dst, send, recv):
        remote(dst, dst, send, recv, (g, e, peer(1))).wait_recv()

    def spread(source, d):
        block = lax.rem(e + E - d, E)
        for k in [1] + [2 * dx for dx in range(1, X)]:
            m = mirror(k)
            go(source, tok.at[m, rows_of(block), :], t_send.at[k, d], t_recv.at[m - 1, d], (g, e, peer(k)))

    for d in range(1, E):
        where = (g, lax.rem(e + d, E), t)
        go(held, held, zt_send.at[d], zt_recv.at[d - 1], where)
    spread(held, 0)
    for d in range(1, E):
        where = (g, lax.rem(e + d, E), t)
        go(ids_all.at[e], ids_all.at[e], zi_send.at[0, d], zi_recv.at[0, d - 1], where)
        go(gates_all.at[e], gates_all.at[e], zi_send.at[1, d], zi_recv.at[1, d - 1], where)
    for k in range(2, T):
        @pl.loop(0, pairs)
        def _(p, k=k):
            fetch(k, p)
    fetch_down(T - 1)

    def from_side(k, d):
        landed = tok.at[k, rows_of(lax.rem(e + E - d, E)), :]
        arrived(landed, t_send.at[k, d], t_recv.at[k - 1, d])
        return landed

    def pass_on(d):
        for k in range(2, T, 2):
            block = lax.rem(e + E - d, E)
            go(
                from_side(k, d), tok.at[k + 1, rows_of(block), :],
                t_send.at[k + 1, d], t_recv.at[k, d], (g, e, peer(1)),
            )

    marks = [2] + [PRE - 5 + 5 * (d - 1) // (E - 2) for d in range(1, E)]
    for d in range(1, E):
        turn_range(marks[d - 1], marks[d])
        if d == E - 1:
            pass_on(0)
        landed = tok.at[0, rows_of(lax.rem(e + E - d, E)), :]
        arrived(landed, zt_send.at[d], zt_recv.at[d - 1])
        spread(landed, d)

    def early(first, last):
        for slot in range(first, last):
            fetched(slot)
        return range(first, last)

    def steps_of(p, n, ks, flip):
        def step(k, f):
            slot = k * pairs + p
            return (
                lambda: tok[k, :, f * TILE:(f + 1) * TILE],
                lambda: pool[slot, n * TILE:(n + 1) * TILE, f * TILE:(f + 1) * TILE] if flip else turned(slot, n, f),
                flip,
            )

        return [step(k, f) for k in ks for f in range(feats // TILE)]

    tiles = tall // TILE

    def sink_of(p, n, first, last):
        def sink(value):
            at = (p, slice(None), slice(n * TILE, (n + 1) * TILE))
            acc[at] = value if first else acc[at] + value
            if last and n == tiles - 1:
                finish(p)

        return sink

    def jobs_of(members, ks, first=False, last=False, flip=False):
        return [
            [
                (steps_of(p, n, ks, flip), sink_of(p, n, first, last))
                for p in members[q::2] for n in range(tiles)
            ]
            for q in range(2)
        ]

    def bands_of(slots):
        return [functools.partial(turn_band, slot, r) for slot in slots for r in range(tall // LANES)]

    low, high = list(range(half)), list(range(half, pairs))
    third, fourth = 2 * pairs, 3 * pairs

    def beside():
        for d in range(E):
            from_side(1, d)
        pass_on(1)

    multiply(jobs_of(low, (0, 1), first=True), LAG, bands_of(early(PRE, third + half)), beside)
    fetch_down(T - 2)
    fetch_down(1)
    pass_on(2)
    multiply(jobs_of(high, (0, 1), first=True), LAG, bands_of(early(third + half, fourth)))
    fetch_down(0)
    for d in range(3, E):
        pass_on(d)
    for d in range(1, E):
        s = lax.rem(e + E - d, E)
        arrived(ids_all.at[s], zi_send.at[0, d], zi_recv.at[0, d - 1])
        arrived(gates_all.at[s], zi_send.at[1, d], zi_recv.at[1, d - 1])
    ids = jnp.concatenate([ids_all[s] for s in range(E)], axis=1)
    gates = jnp.concatenate([gates_all[s] for s in range(E)], axis=1).astype(jnp.float32)
    share = jnp.transpose(gates / jnp.sum(gates, axis=0, keepdims=True))
    ids = jnp.transpose(ids)
    first_of_pair = lax.broadcasted_iota(jnp.int32, (E * tok_rows, wide), 1) < hidden_units

    def finish(p):
        both = acc[p]
        gate, up = both[:, :wide], both[:, wide:]
        weight = [
            jnp.sum(jnp.where(ids == e * experts + 2 * p + j, share, 0.0), axis=1, keepdims=True)
            for j in range(2)
        ]
        value = gate / (1.0 + jnp.exp(-gate)) * up * jnp.where(first_of_pair, weight[0], weight[1])
        hid[:, p * wide:(p + 1) * wide] = value.astype(jnp.bfloat16)

    multiply(jobs_of(low + high, (2,)), LAG, bands_of(early(fourth, fourth + half)))
    for d in range(E):
        from_side(T - 1, d)
    late = high[half // 2:]
    some = early(fourth + half, fourth + half + half // 2)
    for p in late:
        fetched(fourth + p)
    plain, flipped = jobs_of(low, (3,), last=True), jobs_of(late, (3,), last=True, flip=True)
    multiply([plain[q] + flipped[q] for q in range(2)], LAG, bands_of(some))
    multiply(jobs_of(high[:half // 2], (3,), last=True), LAG)

    parts_n = feats // TILE
    def down_jobs(k, n, sinks):
        if n == 0:
            for q in range(half):
                fetched(down_slot[k] + q)

        def step(q, m, f):
            start = m * tall + f * TILE
            return (
                lambda: hid[:, start:start + TILE],
                lambda: pool[
                    down_slot[k] + m, f * TILE:(f + 1) * TILE, (n + q) * TILE:(n + q + 1) * TILE
                ],
                False,
            )

        multiply(
            [[([step(q, m, f) for m in range(half) for f in range(tiles)], sinks(n + q))] for q in range(2)], 0
        )

    def to_side(dx, n):
        def sinks(n):
            def sink(value):
                to_partner[dx, n] = value.astype(jnp.bfloat16)
                go(
                    to_partner.at[dx, n], from_partner.at[dx, n],
                    p_send.at[dx, n], p_recv.at[dx, n], (g, e, peer(1)),
                )

            return sink

        down_jobs(2 * dx + 1, n, sinks)

    def meet_side(dx, n):
        def sinks(n):
            def sink(value):
                arrived(from_partner.at[dx, n], p_send.at[dx, n], p_recv.at[dx, n])
                met = value + from_partner[dx, n].astype(jnp.float32)
                if dx:
                    back = (X - dx) % X
                    to_x[dx, n] = met.astype(jnp.bfloat16)
                    go(
                        to_x.at[dx, n], from_x.at[back, n],
                        x_send.at[dx, n], x_recv.at[back - 1, n], (g, e, peer(2 * dx)),
                    )
                else:
                    own[n] = met

            return sink

        down_jobs(2 * dx, n, sinks)

    for dx in reversed(range(X)):
        for n in range(0, parts_n, 2):
            to_side(dx, n)
        for n in range(0, parts_n, 2):
            meet_side(dx, n)
    for n in range(parts_n):
        for other in range(1, X):
            arrived(from_x.at[other, n], x_send.at[other, n], x_recv.at[other - 1, n])
            own[n] += from_x[other, n].astype(jnp.float32)
        for j in range(1, E):
            to_z[j, n] = own[n, rows_of(lax.rem(e + j, E)), :].astype(jnp.bfloat16)
            go(to_z.at[j, n], from_z.at[j, n], z_send.at[j, n], z_recv.at[j - 1, n], (g, lax.rem(e + j, E), t))
    for n in range(parts_n):
        total = own[n, rows_of(e), :]
        for d in range(1, E):
            arrived(from_z.at[d, n], z_send.at[d, n], z_recv.at[d - 1, n])
            total += from_z[d, n].astype(jnp.float32)
        out_ref[:, n * TILE:(n + 1) * TILE] = total.astype(out_ref.dtype)
    for copy in sent:
        copy.wait_send()


def scratch_of(tok_rows, feats, experts, hidden_units, E, T, per_token):
    bf16, f32, X, N = jnp.bfloat16, jnp.float32, T // 2, E * tok_rows
    parts_n, tall = feats // TILE, 4 * hidden_units
    slots = slots_of(experts, T)
    dma = pltpu.SemaphoreType.DMA
    return [
        ((slots, tall, feats), bf16),
        ((T, N, feats), bf16),
        ((E, per_token, tok_rows), jnp.int32),
        ((E, per_token, tok_rows), jnp.int32),
        ((experts // 2, N, tall), f32),
        ((N, experts * hidden_units), bf16),
        ((X, parts_n, N, TILE), bf16),
        ((X, parts_n, N, TILE), bf16),
        ((X, parts_n, N, TILE), bf16),
        ((X, parts_n, N, TILE), bf16),
        ((E, parts_n, tok_rows, TILE), bf16),
        ((E, parts_n, tok_rows, TILE), bf16),
        ((parts_n, N, TILE), f32),
    ], [
        dma((E - 1,)), dma((2, E - 1)), dma((T - 1, E)), dma((X, parts_n)), dma((X - 1, parts_n)), dma((E - 1, parts_n)),
    ]


def fits_fused(sizes):
    tok_rows, feats, experts, hidden_units, E, T, per_token = sizes
    if T != 4 or E != 4 or experts != 16 or E * tok_rows != 128 or feats % 512 or tok_rows % 16:
        return False
    if 2 * hidden_units % 128 or hidden_units % 16:
        return False
    buffers, _ = scratch_of(*sizes)
    size = 0
    for shape, kind in buffers:
        count = jnp.dtype(kind).itemsize
        for length in shape:
            count *= length
        size += count
    return size < VMEM_BYTES - 1_000_000


def on_device(tokens, expert_ids, gate_fixed, w_gate, w_up, w_down):
    (tok_rows, feats), per_token = tokens.shape, expert_ids.shape[1]
    experts, width, hidden_units = w_gate.shape
    E, T = lax.axis_size("expert"), lax.axis_size("tensor")
    sizes = (tok_rows, feats, experts, hidden_units, E, T, per_token)
    if not fits_fused(sizes):
        return slotted(tokens, expert_ids, gate_fixed, w_gate, w_up, w_down)
    buffers, semaphores = scratch_of(*sizes)
    vmem, anywhere = pl.BlockSpec(memory_space=pltpu.VMEM), pl.BlockSpec(memory_space=pl.ANY)
    return pl.pallas_call(
        functools.partial(fused_kernel, *sizes[:6]),
        out_shape=pltpu.VMEM(tokens.shape, tokens.dtype),
        in_specs=[anywhere] * 6,
        out_specs=vmem,
        scratch_shapes=[pltpu.VMEM(shape, kind) for shape, kind in buffers] + semaphores,
        compiler_params=pltpu.CompilerParams(
            collective_id=0, has_side_effects=True, vmem_limit_bytes=VMEM_BYTES
        ),
    )(
        tokens,
        expert_ids.T,
        gate_fixed.T,
        jnp.swapaxes(w_gate, 1, 2),
        jnp.swapaxes(w_up, 1, 2),
        w_down.reshape(experts * hidden_units, width),
    )


def solution(mesh):
    placed = (
        P(("groups", "expert"), "tensor"),
        P(("groups", "expert"), None),
        P(("groups", "expert"), None),
        P("expert", None, "tensor"),
        P("expert", None, "tensor"),
        P("expert", "tensor", None),
    )
    return jax.shard_map(
        on_device,
        mesh=mesh,
        in_specs=placed,
        out_specs=P(("groups", "expert"), "tensor"),
        check_vma=False,
    )
```

```python
import functools

import jax
import jax.numpy as jnp
from jax import lax
from jax.experimental import pallas as pl
from jax.experimental.pallas import tpu as pltpu
from jax.sharding import PartitionSpec as P

CAP = 8


def expert_block(slot_rows, w_gate, w_up, w_down):
    gate_proj = jnp.einsum("gekd,edf->gekf", slot_rows, w_gate, preferred_element_type=jnp.float32)
    up_proj = jnp.einsum("gekd,edf->gekf", slot_rows, w_up, preferred_element_type=jnp.float32)
    hidden = (jax.nn.silu(gate_proj) * up_proj).astype(jnp.bfloat16)
    partial_value = jnp.einsum("gekf,efd->gekd", hidden, w_down, preferred_element_type=jnp.float32)
    summed = lax.psum_scatter(
        partial_value.astype(jnp.bfloat16), "tensor", scatter_dimension=3, tiled=True
    )
    return lax.all_to_all(summed, "expert", split_axis=0, concat_axis=0, tiled=True)


def slotted(tokens, expert_ids, gate_fixed, w_gate, w_up, w_down):
    tok_rows, per_token = expert_ids.shape
    local_experts = w_gate.shape[0]
    devices_e = lax.axis_size("expert")
    experts = local_experts * devices_e
    capacity = CAP
    flat_ids = expert_ids.reshape(-1)
    pick_count = tok_rows * per_token
    onehot = (flat_ids[:, None] == jnp.arange(experts, dtype=jnp.int32)[None, :]).astype(jnp.int32)
    before = jnp.cumsum(onehot, axis=0) - onehot
    slot_rank = jnp.sum(before * onehot, axis=1)
    slot_index = flat_ids * capacity + slot_rank
    owner_row = jnp.arange(pick_count, dtype=jnp.int32) // per_token
    slot_token = jnp.full((experts * capacity,), tok_rows, jnp.int32).at[slot_index].set(owner_row)
    padded = jnp.concatenate([tokens, jnp.zeros((1, tokens.shape[1]), tokens.dtype)], axis=0)
    returned = expert_block(
        lax.all_gather(
            lax.all_to_all(
                padded[slot_token].reshape(devices_e, local_experts, capacity, tokens.shape[1]),
                "expert",
                split_axis=0,
                concat_axis=0,
                tiled=True,
            ),
            "tensor",
            axis=3,
            tiled=True,
        ),
        w_gate,
        w_up,
        w_down,
    )
    flat_returned = returned.reshape(experts * capacity, returned.shape[3])
    picked = flat_returned[slot_index].reshape(tok_rows, per_token, returned.shape[3])
    weights = gate_fixed.astype(jnp.float32)
    gate_share = weights / jnp.sum(weights, axis=1, keepdims=True)
    mixed_out = jnp.einsum("tk,tkf->tf", gate_share, picked.astype(jnp.float32))
    return mixed_out.astype(jnp.bfloat16)


MESH = pl.DeviceIdType.MESH
VMEM_BYTES = 66_500_000
LANES = 128
TILE = 256
CUT = 128
CUTS = TILE // CUT
SUMS = 6
LAG = 1
PRE = 16


def fused_kernel(*args):
    tok_rows, feats, experts, _, E, T = args[:6]
    shape, parts_n, dma = (tok_rows * E, TILE), feats // TILE, pltpu.SemaphoreType.DMA

    def body(*scoped):
        fused_body(scoped[:SUMS], scoped[SUMS:2 * SUMS], scoped[2 * SUMS:], *args)

    pl.run_scoped(
        body, *[pltpu.ACC(q)(shape, jnp.float32) for q in range(2) for _ in range(SUMS)],
        dma((slots_of(experts, T),)), dma((3,)), dma((E,)), dma((2, E)), dma((T, E)),
        dma((T // 2, parts_n)), dma((T // 2, CUTS * parts_n)), dma((E, CUTS * parts_n)),
        dma((2, E)), dma,
    )


def slots_of(experts, T):
    return T * experts // 2 + experts // 4


def fused_body(
    sums0, sums1, local_sems, tok_rows, feats, experts, hidden_units, E, T,
    x_ref, ids_ref, gates_ref, wg_ref, wu_ref, wd_ref, out_ref,
    pool, tok, ids_all, gates_all, acc, hid,
    to_partner, from_partner, to_x, from_x, to_z, from_z, own, ids_t, share_t,
    edge, to_edge, from_edge, to_far, from_far,
    zt_recv, zi_recv, t_recv, p_recv, x_recv, z_recv, edge_recv, far_recv,
):
    w_sem, own_sem, zt_send, zi_send, t_send, p_send, x_send, z_send, edge_send, far_send = local_sems
    g, e, t = lax.axis_index("groups"), lax.axis_index("expert"), lax.axis_index("tensor")
    X = T // 2
    x, c = lax.div(t, 2), lax.rem(t, 2)
    pairs, half = experts // 2, experts // 4
    wide = 2 * hidden_units
    tall = 2 * wide

    def peer(k):
        half_k, side = k // 2, k % 2
        return lax.rem(x + half_k, X) * 2 + lax.rem(c + side, 2)

    def mirror(k):
        return (-(k // 2)) % X * 2 + k % 2

    def rows_of(block):
        return pl.ds(pl.multiple_of(block * tok_rows, tok_rows), tok_rows)

    def features_of(k):
        return pl.ds(pl.multiple_of(peer(k) * feats, feats), feats)

    def fetch(k, p):
        slot = k * pairs + p
        for part, w in enumerate((wg_ref, wu_ref)):
            for j in range(2):
                pltpu.make_async_copy(
                    w.at[2 * p + j, :, features_of(k)],
                    pool.at[slot, pl.ds(part * wide + j * hidden_units, hidden_units), :],
                    w_sem.at[slot],
                ).start()

    def fetched(slot):
        pltpu.make_async_copy(pool.at[slot], pool.at[slot], w_sem.at[slot]).wait()

    down_slot = {T - 1: T * pairs, T - 2: 0, 1: pairs, 0: half}

    def fetch_down(k):
        for q in range(half):
            slot = down_slot[k] + q
            pltpu.make_async_copy(
                wd_ref.at[pl.ds(q * tall, tall), features_of(k)], pool.at[slot], w_sem.at[slot]
            ).start()

    def turn_piece(slot, r, f):
        at = (slot, slice(r * LANES, (r + 1) * LANES), slice(f * TILE, (f + 1) * TILE))
        piece = pool[at]
        pool[at] = jnp.concatenate(
            [jnp.transpose(piece[:, j * LANES:(j + 1) * LANES]) for j in range(TILE // LANES)], axis=1
        )

    def turn(slot):
        for r in range(tall // LANES):
            for f in range(feats // TILE):
                turn_piece(slot, r, f)

    def turned(slot, n, f):
        bands = [
            pool[slot, (2 * n + r) * LANES:(2 * n + r + 1) * LANES, f * TILE:(f + 1) * TILE] for r in range(2)
        ]
        return jnp.concatenate(
            [jnp.concatenate([band[:, j * LANES:(j + 1) * LANES] for band in bands], axis=1) for j in range(2)],
            axis=0,
        )

    sums, stage, turn_of, beside = (sums0, sums1), [0, 0], [0, 0], []

    def multiply(jobs, lag, side=(), pause=None, cut=0, keep=False):
        beside.extend(side)
        left = sum(len(steps) for steps, _ in jobs[0])
        waiting = []

        def run(pair, used, steps):
            nonlocal left
            for s in steps:
                rows = pair[0][0][s][0]()
                for q in range(2):
                    _, weights, flip = pair[q][0][s]
                    at = stage[q] % 2
                    stage[q] += 1
                    pltpu.matmul_push_rhs(weights(), staging_register=at, mxu_index=q, transpose=flip)
                    pltpu.matmul_acc_lhs(used[q], rows, load_staged_rhs=at)
                for _ in range(-(-len(beside) // left)):
                    beside.pop(0)()
                left -= 1

        def drain(limit):
            while len(waiting) > limit:
                for sink, used_sum in waiting.pop(0):
                    sink(pltpu.matmul_pop(used_sum))

        pairs_of = list(zip(*jobs))
        uses = []
        for _ in pairs_of:
            uses.append([sums[q][turn_of[q] % SUMS] for q in range(2)])
            for q in range(2):
                turn_of[q] += 1
        whole = left
        if cut and pause is None:
            left = cut * len(pairs_of)
        for pair, used in zip(pairs_of, uses):
            run(pair, used, range(cut))
        left = whole - cut * len(pairs_of)
        if pause is not None:
            pause()
        for pair, used in zip(pairs_of, uses):
            run(pair, used, range(cut, len(pair[0][0])))
            waiting.append([(pair[q][1], used[q]) for q in range(2)])
            drain(lag)
        drain(0)
        while beside and not keep:
            beside.pop(0)()

    local = [
        pltpu.make_async_copy(x_ref, tok.at[0, rows_of(e), :], own_sem.at[0]),
        pltpu.make_async_copy(ids_ref, ids_all.at[e], own_sem.at[1]),
        pltpu.make_async_copy(gates_ref, gates_all.at[e], own_sem.at[2]),
    ]
    for copy in local:
        copy.start()
    for k in range(2):
        @pl.loop(0, pairs)
        def _(p, k=k):
            fetch(k, p)

    barrier = pltpu.get_barrier_semaphore()
    for d in range(1, E):
        pl.semaphore_signal(barrier, inc=1, device_id=(g, lax.rem(e + d, E), t), device_id_type=MESH)
    for k in range(1, T):
        pl.semaphore_signal(barrier, inc=1, device_id=(g, e, peer(k)), device_id_type=MESH)

    def turn_range(first, last):
        @pl.loop(first, last)
        def _(slot):
            fetched(slot)
            turn(slot)

    turn_range(0, 2)
    pl.semaphore_wait(barrier, E - 1 + T - 1)

    def remote(src, dst, send, recv, where):
        return pltpu.make_async_remote_copy(
            src_ref=src, dst_ref=dst, send_sem=send, recv_sem=recv, device_id=where, device_id_type=MESH
        )

    for copy in local:
        copy.wait()
    held = tok.at[0, rows_of(e), :]
    sent = []

    def go(*args):
        copy = remote(*args)
        copy.start()
        sent.append(copy)

    def arrived(dst, send, recv):
        remote(dst, dst, send, recv, (g, e, peer(1))).wait_recv()

    def spread(source, d):
        block = lax.rem(e + E - d, E)
        for k in [1] + [2 * dx for dx in range(1, X)]:
            m = mirror(k)
            go(source, tok.at[m, rows_of(block), :], t_send.at[k, d], t_recv.at[m - 1, d], (g, e, peer(k)))

    for d in range(1, E):
        where = (g, lax.rem(e + d, E), t)
        go(held, held, zt_send.at[d], zt_recv.at[d - 1], where)
    spread(held, 0)
    for d in range(1, E):
        where = (g, lax.rem(e + d, E), t)
        go(ids_all.at[e], ids_all.at[e], zi_send.at[0, d], zi_recv.at[0, d - 1], where)
        go(gates_all.at[e], gates_all.at[e], zi_send.at[1, d], zi_recv.at[1, d - 1], where)
    for k in range(2, T):
        @pl.loop(0, pairs)
        def _(p, k=k):
            fetch(k, p)
    fetch_down(T - 1)

    def from_side(k, d):
        landed = tok.at[k, rows_of(lax.rem(e + E - d, E)), :]
        arrived(landed, t_send.at[k, d], t_recv.at[k - 1, d])
        return landed

    def pass_on(d):
        for k in range(2, T, 2):
            block = lax.rem(e + E - d, E)
            go(
                from_side(k, d), tok.at[k + 1, rows_of(block), :],
                t_send.at[k + 1, d], t_recv.at[k, d], (g, e, peer(1)),
            )

    marks = [2] + [PRE - 5 + 5 * (d - 1) // (E - 2) for d in range(1, E)]
    for d in range(1, E):
        turn_range(marks[d - 1], marks[d])
        if d == E - 1:
            pass_on(0)
        landed = tok.at[0, rows_of(lax.rem(e + E - d, E)), :]
        arrived(landed, zt_send.at[d], zt_recv.at[d - 1])
        spread(landed, d)

    def early(first, last):
        for slot in range(first, last):
            fetched(slot)
        return range(first, last)

    def steps_of(p, n, ks, flip):
        def step(k, f):
            slot = k * pairs + p
            return (
                lambda: tok[k, :, f * TILE:(f + 1) * TILE],
                lambda: pool[slot, n * TILE:(n + 1) * TILE, f * TILE:(f + 1) * TILE] if flip else turned(slot, n, f),
                flip,
            )

        return [step(k, f) for k in ks for f in range(feats // TILE)]

    tiles = tall // TILE

    def sink_of(p, n, first, last):
        def sink(value):
            at = (p, slice(None), slice(n * TILE, (n + 1) * TILE))
            acc[at] = value if first else acc[at] + value
            if last and n == tiles - 1:
                finish(p)

        return sink

    def jobs_of(members, ks, first=False, last=False, flip=False):
        return [
            [
                (steps_of(p, n, ks, flip), sink_of(p, n, first, last))
                for p in members[q::2] for n in range(tiles)
            ]
            for q in range(2)
        ]

    def bands_of(slots):
        return [
            functools.partial(turn_piece, slot, r, f)
            for slot in slots for r in range(tall // LANES) for f in range(feats // TILE)
        ]

    low, high = list(range(half)), list(range(half, pairs))
    third, fourth = 2 * pairs, 3 * pairs

    def between():
        for d in range(E):
            from_side(1, d)
        pass_on(1)

    multiply(jobs_of(low, (0, 1), first=True), LAG, bands_of(early(PRE, third + half)), between, feats // TILE)
    fetch_down(T - 2)
    fetch_down(1)
    pass_on(2)
    multiply(jobs_of(high, (0, 1), first=True), LAG, bands_of(early(third + half, fourth)))
    fetch_down(0)
    for d in range(3, E):
        pass_on(d)
    for d in range(1, E):
        s = lax.rem(e + E - d, E)
        arrived(ids_all.at[s], zi_send.at[0, d], zi_recv.at[0, d - 1])
        arrived(gates_all.at[s], zi_send.at[1, d], zi_recv.at[1, d - 1])
    ids = jnp.concatenate([ids_all[s] for s in range(E)], axis=1)
    gates = jnp.concatenate([gates_all[s] for s in range(E)], axis=1).astype(jnp.float32)
    share_t[...] = jnp.transpose(gates / jnp.sum(gates, axis=0, keepdims=True))
    ids_t[...] = jnp.transpose(ids)
    band = 32

    def finish_band(p, start):
        rows = slice(start, start + band)
        gate, up = acc[p, rows, :wide], acc[p, rows, wide:]
        weight = [
            jnp.sum(
                jnp.where(ids_t[rows] == e * experts + 2 * p + j, share_t[rows], 0.0), axis=1, keepdims=True
            )
            for j in range(2)
        ]
        first = lax.broadcasted_iota(jnp.int32, (band, wide), 1) < hidden_units
        value = gate / (1.0 + jnp.exp(-gate)) * up * jnp.where(first, weight[0], weight[1])
        hid[rows, p * wide:(p + 1) * wide] = value.astype(jnp.bfloat16)

    def finish(p):
        beside.extend(functools.partial(finish_band, p, start) for start in range(0, E * tok_rows, band))

    multiply(jobs_of(low + high, (2,)), LAG, bands_of(early(fourth, fourth + half)))
    for d in range(E):
        from_side(T - 1, d)
    late = high[half // 2:]
    some = early(fourth + half, fourth + half + half // 2)
    for p in late:
        fetched(fourth + p)
    plain, flipped = jobs_of(low, (3,), last=True), jobs_of(late, (3,), last=True, flip=True)
    multiply([plain[q] + flipped[q] for q in range(2)], LAG, bands_of(some), keep=True)
    parts_n = feats // TILE
    def down_ready(k):
        for q in range(half):
            fetched(down_slot[k] + q)

    def down_jobs(k, ns, sink_at, order=None):
        def step(n, m):
            start = m * TILE
            slot, f = down_slot[k] + m // tiles, m % tiles
            return (
                lambda: hid[:, start:start + TILE],
                lambda: pool[slot, f * TILE:(f + 1) * TILE, n * TILE:(n + 1) * TILE],
                False,
            )

        order = range(half * tiles) if order is None else order
        return [[([step(n + q, m) for m in order], sink_at(n + q)) for n in ns] for q in range(2)]

    def side_sink(dx):
        def sink_at(n):
            def sink(value):
                to_partner[dx, n] = value.astype(jnp.bfloat16)
                go(
                    to_partner.at[dx, n], from_partner.at[dx, n],
                    p_send.at[dx, n], p_recv.at[dx, n], (g, e, peer(1)),
                )

            return sink

        return sink_at

    def across_z(dx, met):
        edge[dx] = met
        for j in range(1, E):
            to_edge[dx, j] = edge[dx, rows_of(lax.rem(e + j, E)), :].astype(jnp.bfloat16)
            go(
                to_edge.at[dx, j], from_edge.at[dx, j],
                edge_send.at[dx, j], edge_recv.at[dx, j - 1], (g, lax.rem(e + j, E), t),
            )

    def gathered_edge(dx):
        total = edge[dx, rows_of(e), :]
        for d in range(1, E):
            arrived(from_edge.at[dx, d], edge_send.at[dx, d], edge_recv.at[dx, d - 1])
            total += from_edge[dx, d].astype(jnp.float32)
        return total

    def meet_sink(dx):
        def sink_at(n):
            def sink(value):
                arrived(from_partner.at[dx, n], p_send.at[dx, n], p_recv.at[dx, n])
                met = value + from_partner[dx, n].astype(jnp.float32)
                if n == parts_n - 1:
                    across_z(dx, met)
                    return
                if not dx:
                    own[n] = met
                    return
                back = (X - dx) % X
                for j in range(CUTS):
                    m = n * CUTS + j
                    to_x[dx, m] = met[:, j * CUT:(j + 1) * CUT].astype(jnp.bfloat16)
                    go(
                        to_x.at[dx, m], from_x.at[back, m],
                        x_send.at[dx, m], x_recv.at[back - 1, m], (g, e, peer(2 * dx)),
                    )

            return sink

        return sink_at

    open_pairs = range(min(high) * wide // TILE, (min(high) + half // 2) * wide // TILE)
    order = [m for m in range(half * tiles) if m not in open_pairs] + list(open_pairs)
    down_ready(T - 1)
    multiply(jobs_of(high[:half // 2], (3,), last=True), LAG, keep=True)
    multiply(
        down_jobs(T - 1, range(0, parts_n, 2), side_sink(X - 1), order), 0, cut=len(order) - len(open_pairs)
    )
    for dx in reversed(range(X)):
        if dx < X - 1:
            down_ready(2 * dx + 1)
            for n in reversed(range(0, parts_n, 2)):
                multiply(down_jobs(2 * dx + 1, [n], side_sink(dx)), 0)
        down_ready(2 * dx)
        for n in range(0, parts_n, 2) if dx else reversed(range(0, parts_n, 2)):
            multiply(down_jobs(2 * dx, [n], meet_sink(dx)), 0)
    inner = (parts_n - 1) * CUTS
    for m in range(inner):
        n, columns = m // CUTS, slice(m % CUTS * CUT, (m % CUTS + 1) * CUT)
        for other in range(1, X):
            arrived(from_x.at[other, m], x_send.at[other, m], x_recv.at[other - 1, m])
            own[n, :, columns] += from_x[other, m].astype(jnp.float32)
        for j in range(1, E):
            to_z[j, m] = own[n, rows_of(lax.rem(e + j, E)), columns].astype(jnp.bfloat16)
            go(to_z.at[j, m], from_z.at[j, m], z_send.at[j, m], z_recv.at[j - 1, m], (g, lax.rem(e + j, E), t))
        if m == inner - CUTS:
            to_far[...] = gathered_edge(1).astype(jnp.bfloat16)
            go(to_far, from_far, far_send, far_recv, (g, e, peer(2)))
    for m in range(inner):
        n, columns = m // CUTS, slice(m % CUTS * CUT, (m % CUTS + 1) * CUT)
        total = own[n, rows_of(e), columns]
        for d in range(1, E):
            arrived(from_z.at[d, m], z_send.at[d, m], z_recv.at[d - 1, m])
            total += from_z[d, m].astype(jnp.float32)
        out_ref[:, m * CUT:(m + 1) * CUT] = total.astype(out_ref.dtype)
        if m == inner - 2:
            total = gathered_edge(0)
            arrived(from_far, far_send, far_recv)
            total += from_far[...].astype(jnp.float32)
            out_ref[:, inner * CUT:] = total.astype(out_ref.dtype)
    for copy in sent:
        copy.wait_send()


def scratch_of(tok_rows, feats, experts, hidden_units, E, T, per_token):
    bf16, f32, X, N = jnp.bfloat16, jnp.float32, T // 2, E * tok_rows
    parts_n, cuts_n, tall = feats // TILE, feats // CUT, 4 * hidden_units
    slots = slots_of(experts, T)
    dma = pltpu.SemaphoreType.DMA
    return [
        ((slots, tall, feats), bf16),
        ((T, N, feats), bf16),
        ((E, per_token, tok_rows), jnp.int32),
        ((E, per_token, tok_rows), jnp.int32),
        ((experts // 2, N, tall), f32),
        ((N, experts * hidden_units), bf16),
        ((X, parts_n, N, TILE), bf16),
        ((X, parts_n, N, TILE), bf16),
        ((X, cuts_n - CUTS, N, CUT), bf16),
        ((X, cuts_n - CUTS, N, CUT), bf16),
        ((E, cuts_n - CUTS, tok_rows, CUT), bf16),
        ((E, cuts_n - CUTS, tok_rows, CUT), bf16),
        ((parts_n - 1, N, TILE), f32),
        ((N, per_token), jnp.int32),
        ((N, per_token), f32),
        ((X, N, TILE), f32),
        ((X, E, tok_rows, TILE), bf16),
        ((X, E, tok_rows, TILE), bf16),
        ((tok_rows, TILE), bf16),
        ((tok_rows, TILE), bf16),
    ], [
        dma((E - 1,)), dma((2, E - 1)), dma((T - 1, E)), dma((X, parts_n)), dma((X - 1, cuts_n - CUTS)), dma((E - 1, cuts_n - CUTS)),
        dma((X, E - 1)), dma,
    ]


def fits_fused(sizes):
    tok_rows, feats, experts, hidden_units, E, T, per_token = sizes
    if T != 4 or E != 4 or experts != 16 or E * tok_rows != 128 or feats % 512 or tok_rows % 16:
        return False
    if 2 * hidden_units % 128 or hidden_units % 16:
        return False
    buffers, _ = scratch_of(*sizes)
    size = 0
    for shape, kind in buffers:
        count = jnp.dtype(kind).itemsize
        for length in shape:
            count *= length
        size += count
    return size < VMEM_BYTES - 1_000_000


def on_device(tokens, expert_ids, gate_fixed, w_gate, w_up, w_down):
    (tok_rows, feats), per_token = tokens.shape, expert_ids.shape[1]
    experts, width, hidden_units = w_gate.shape
    E, T = lax.axis_size("expert"), lax.axis_size("tensor")
    sizes = (tok_rows, feats, experts, hidden_units, E, T, per_token)
    if not fits_fused(sizes):
        return slotted(tokens, expert_ids, gate_fixed, w_gate, w_up, w_down)
    buffers, semaphores = scratch_of(*sizes)
    vmem, anywhere = pl.BlockSpec(memory_space=pltpu.VMEM), pl.BlockSpec(memory_space=pl.ANY)
    return pl.pallas_call(
        functools.partial(fused_kernel, *sizes[:6]),
        out_shape=pltpu.VMEM(tokens.shape, tokens.dtype),
        in_specs=[anywhere] * 6,
        out_specs=vmem,
        scratch_shapes=[pltpu.VMEM(shape, kind) for shape, kind in buffers] + semaphores,
        compiler_params=pltpu.CompilerParams(
            collective_id=0, has_side_effects=True, vmem_limit_bytes=VMEM_BYTES,
        ),
    )(
        tokens,
        expert_ids.T,
        gate_fixed.T,
        jnp.swapaxes(w_gate, 1, 2),
        jnp.swapaxes(w_up, 1, 2),
        w_down.reshape(experts * hidden_units, width),
    )


def solution(mesh):
    placed = (
        P(("groups", "expert"), "tensor"),
        P(("groups", "expert"), None),
        P(("groups", "expert"), None),
        P("expert", None, "tensor"),
        P("expert", None, "tensor"),
        P("expert", "tensor", None),
    )
    return jax.shard_map(
        on_device,
        mesh=mesh,
        in_specs=placed,
        out_specs=P(("groups", "expert"), "tensor"),
        check_vma=False,
    )
```

```python
import functools

import jax
import jax.numpy as jnp
from jax import lax
from jax.experimental import pallas as pl
from jax.experimental.pallas import tpu as pltpu
from jax.sharding import PartitionSpec as P

CAP = 8


def expert_block(slot_rows, w_gate, w_up, w_down):
    gate_proj = jnp.einsum("gekd,edf->gekf", slot_rows, w_gate, preferred_element_type=jnp.float32)
    up_proj = jnp.einsum("gekd,edf->gekf", slot_rows, w_up, preferred_element_type=jnp.float32)
    hidden = (jax.nn.silu(gate_proj) * up_proj).astype(jnp.bfloat16)
    partial_value = jnp.einsum("gekf,efd->gekd", hidden, w_down, preferred_element_type=jnp.float32)
    summed = lax.psum_scatter(
        partial_value.astype(jnp.bfloat16), "tensor", scatter_dimension=3, tiled=True
    )
    return lax.all_to_all(summed, "expert", split_axis=0, concat_axis=0, tiled=True)


def slotted(tokens, expert_ids, gate_fixed, w_gate, w_up, w_down):
    tok_rows, per_token = expert_ids.shape
    local_experts = w_gate.shape[0]
    devices_e = lax.axis_size("expert")
    experts = local_experts * devices_e
    capacity = CAP
    flat_ids = expert_ids.reshape(-1)
    pick_count = tok_rows * per_token
    onehot = (flat_ids[:, None] == jnp.arange(experts, dtype=jnp.int32)[None, :]).astype(jnp.int32)
    before = jnp.cumsum(onehot, axis=0) - onehot
    slot_rank = jnp.sum(before * onehot, axis=1)
    slot_index = flat_ids * capacity + slot_rank
    owner_row = jnp.arange(pick_count, dtype=jnp.int32) // per_token
    slot_token = jnp.full((experts * capacity,), tok_rows, jnp.int32).at[slot_index].set(owner_row)
    padded = jnp.concatenate([tokens, jnp.zeros((1, tokens.shape[1]), tokens.dtype)], axis=0)
    returned = expert_block(
        lax.all_gather(
            lax.all_to_all(
                padded[slot_token].reshape(devices_e, local_experts, capacity, tokens.shape[1]),
                "expert",
                split_axis=0,
                concat_axis=0,
                tiled=True,
            ),
            "tensor",
            axis=3,
            tiled=True,
        ),
        w_gate,
        w_up,
        w_down,
    )
    flat_returned = returned.reshape(experts * capacity, returned.shape[3])
    picked = flat_returned[slot_index].reshape(tok_rows, per_token, returned.shape[3])
    weights = gate_fixed.astype(jnp.float32)
    gate_share = weights / jnp.sum(weights, axis=1, keepdims=True)
    mixed_out = jnp.einsum("tk,tkf->tf", gate_share, picked.astype(jnp.float32))
    return mixed_out.astype(jnp.bfloat16)


MESH = pl.DeviceIdType.MESH
VMEM_BYTES = 66_500_000
LANES = 128
TILE = 256
CUT = 128
CUTS = TILE // CUT
SUMS = 6
LAG = 1
PRE = 16


def fused_kernel(*args):
    tok_rows, feats, experts, _, E, T = args[:6]
    shape, parts_n, dma = (tok_rows * E, TILE), feats // TILE, pltpu.SemaphoreType.DMA

    def body(*scoped):
        fused_body(scoped[:SUMS], scoped[SUMS:2 * SUMS], scoped[2 * SUMS:], *args)

    pl.run_scoped(
        body, *[pltpu.ACC(q)(shape, jnp.float32) for q in range(2) for _ in range(SUMS)],
        dma((slots_of(experts, T),)), dma((3,)), dma((E,)), dma((2, E)), dma((T, E)),
        dma((T // 2, parts_n)), dma((T // 2, CUTS * parts_n)), dma((E, CUTS * parts_n)),
        dma((2, E)), dma,
    )


def slots_of(experts, T):
    return T * experts // 2 + experts // 4


def fused_body(
    sums0, sums1, local_sems, tok_rows, feats, experts, hidden_units, E, T,
    x_ref, ids_ref, gates_ref, wg_ref, wu_ref, wd_ref, out_ref,
    pool, tok, ids_all, gates_all, acc, hid,
    to_partner, from_partner, to_x, from_x, to_z, from_z, own, ids_t, share_t,
    edge, to_edge, from_edge, to_far, from_far,
    zt_recv, zi_recv, t_recv, p_recv, x_recv, z_recv, edge_recv, far_recv,
):
    w_sem, own_sem, zt_send, zi_send, t_send, p_send, x_send, z_send, edge_send, far_send = local_sems
    g, e, t = lax.axis_index("groups"), lax.axis_index("expert"), lax.axis_index("tensor")
    X = T // 2
    x, c = lax.div(t, 2), lax.rem(t, 2)
    pairs, half = experts // 2, experts // 4
    wide = 2 * hidden_units
    tall = 2 * wide

    def peer(k):
        half_k, side = k // 2, k % 2
        return lax.rem(x + half_k, X) * 2 + lax.rem(c + side, 2)

    def mirror(k):
        return (-(k // 2)) % X * 2 + k % 2

    def rows_of(block):
        return pl.ds(pl.multiple_of(block * tok_rows, tok_rows), tok_rows)

    def features_of(k):
        return pl.ds(pl.multiple_of(peer(k) * feats, feats), feats)

    def fetch(k, p):
        slot = k * pairs + p
        for part, w in enumerate((wg_ref, wu_ref)):
            for j in range(2):
                pltpu.make_async_copy(
                    w.at[2 * p + j, :, features_of(k)],
                    pool.at[slot, pl.ds(part * wide + j * hidden_units, hidden_units), :],
                    w_sem.at[slot],
                ).start()

    def fetched(slot):
        pltpu.make_async_copy(pool.at[slot], pool.at[slot], w_sem.at[slot]).wait()

    down_slot = {T - 1: T * pairs, T - 2: 0, 1: pairs, 0: half}

    def fetch_down(k):
        for q in range(half):
            slot = down_slot[k] + q
            pltpu.make_async_copy(
                wd_ref.at[pl.ds(q * tall, tall), features_of(k)], pool.at[slot], w_sem.at[slot]
            ).start()

    def turn_piece(slot, r, f):
        at = (slot, slice(r * LANES, (r + 1) * LANES), slice(f * TILE, (f + 1) * TILE))
        piece = pool[at]
        pool[at] = jnp.concatenate(
            [jnp.transpose(piece[:, j * LANES:(j + 1) * LANES]) for j in range(TILE // LANES)], axis=1
        )

    def turn(slot):
        for r in range(tall // LANES):
            for f in range(feats // TILE):
                turn_piece(slot, r, f)

    def turned(slot, n, f):
        bands = [
            pool[slot, (2 * n + r) * LANES:(2 * n + r + 1) * LANES, f * TILE:(f + 1) * TILE] for r in range(2)
        ]
        return jnp.concatenate(
            [jnp.concatenate([band[:, j * LANES:(j + 1) * LANES] for band in bands], axis=1) for j in range(2)],
            axis=0,
        )

    sums, stage, turn_of, beside = (sums0, sums1), [0, 0], [0, 0], []

    def multiply(jobs, lag, side=(), pause=None, cut=0, keep=False):
        beside.extend(side)
        left = sum(len(steps) for steps, _ in jobs[0])
        waiting = []

        def run(pair, used, steps):
            nonlocal left
            for s in steps:
                rows = pair[0][0][s][0]()
                for q in range(2):
                    _, weights, flip = pair[q][0][s]
                    at = stage[q] % 2
                    stage[q] += 1
                    pltpu.matmul_push_rhs(weights(), staging_register=at, mxu_index=q, transpose=flip)
                    pltpu.matmul_acc_lhs(used[q], rows, load_staged_rhs=at)
                for _ in range(-(-len(beside) // left)):
                    beside.pop(0)()
                left -= 1

        def drain(limit):
            while len(waiting) > limit:
                for sink, used_sum in waiting.pop(0):
                    sink(pltpu.matmul_pop(used_sum))

        pairs_of = list(zip(*jobs))
        uses = []
        for _ in pairs_of:
            uses.append([sums[q][turn_of[q] % SUMS] for q in range(2)])
            for q in range(2):
                turn_of[q] += 1
        whole = left
        if cut and pause is None:
            left = cut * len(pairs_of)
        for pair, used in zip(pairs_of, uses):
            run(pair, used, range(cut))
        left = whole - cut * len(pairs_of)
        if pause is not None:
            pause()
        for pair, used in zip(pairs_of, uses):
            run(pair, used, range(cut, len(pair[0][0])))
            waiting.append([(pair[q][1], used[q]) for q in range(2)])
            drain(lag)
        drain(0)
        while beside and not keep:
            beside.pop(0)()

    local = [
        pltpu.make_async_copy(x_ref, tok.at[0, rows_of(e), :], own_sem.at[0]),
        pltpu.make_async_copy(ids_ref, ids_all.at[e], own_sem.at[1]),
        pltpu.make_async_copy(gates_ref, gates_all.at[e], own_sem.at[2]),
    ]
    for copy in local:
        copy.start()
    for k in range(2):
        @pl.loop(0, pairs)
        def _(p, k=k):
            fetch(k, p)

    barrier = pltpu.get_barrier_semaphore()
    for d in range(1, E):
        pl.semaphore_signal(barrier, inc=1, device_id=(g, lax.rem(e + d, E), t), device_id_type=MESH)
    for k in range(1, T):
        pl.semaphore_signal(barrier, inc=1, device_id=(g, e, peer(k)), device_id_type=MESH)

    def turn_range(first, last):
        @pl.loop(first, last)
        def _(slot):
            fetched(slot)
            turn(slot)

    turn_range(0, 2)
    pl.semaphore_wait(barrier, E - 1 + T - 1)

    def remote(src, dst, send, recv, where):
        return pltpu.make_async_remote_copy(
            src_ref=src, dst_ref=dst, send_sem=send, recv_sem=recv, device_id=where, device_id_type=MESH
        )

    for copy in local:
        copy.wait()
    held = tok.at[0, rows_of(e), :]
    sent = []

    def go(*args):
        copy = remote(*args)
        copy.start()
        sent.append(copy)

    def arrived(dst, send, recv):
        remote(dst, dst, send, recv, (g, e, peer(1))).wait_recv()

    def spread(source, d):
        block = lax.rem(e + E - d, E)
        for k in [1] + [2 * dx for dx in range(1, X)]:
            m = mirror(k)
            go(source, tok.at[m, rows_of(block), :], t_send.at[k, d], t_recv.at[m - 1, d], (g, e, peer(k)))

    for d in range(1, E):
        where = (g, lax.rem(e + d, E), t)
        go(held, held, zt_send.at[d], zt_recv.at[d - 1], where)
    spread(held, 0)
    for d in range(1, E):
        where = (g, lax.rem(e + d, E), t)
        go(ids_all.at[e], ids_all.at[e], zi_send.at[0, d], zi_recv.at[0, d - 1], where)
        go(gates_all.at[e], gates_all.at[e], zi_send.at[1, d], zi_recv.at[1, d - 1], where)
    for k in range(2, T):
        @pl.loop(0, pairs)
        def _(p, k=k):
            fetch(k, p)
    fetch_down(T - 1)

    def from_side(k, d):
        landed = tok.at[k, rows_of(lax.rem(e + E - d, E)), :]
        arrived(landed, t_send.at[k, d], t_recv.at[k - 1, d])
        return landed

    def pass_on(d):
        for k in range(2, T, 2):
            block = lax.rem(e + E - d, E)
            go(
                from_side(k, d), tok.at[k + 1, rows_of(block), :],
                t_send.at[k + 1, d], t_recv.at[k, d], (g, e, peer(1)),
            )

    def routing():
        for d in range(1, E):
            s = lax.rem(e + E - d, E)
            arrived(ids_all.at[s], zi_send.at[0, d], zi_recv.at[0, d - 1])
            arrived(gates_all.at[s], zi_send.at[1, d], zi_recv.at[1, d - 1])
        ids = jnp.concatenate([ids_all[s] for s in range(E)], axis=1)
        gates = jnp.concatenate([gates_all[s] for s in range(E)], axis=1).astype(jnp.float32)
        share_t[...] = jnp.transpose(gates / jnp.sum(gates, axis=0, keepdims=True))
        ids_t[...] = jnp.transpose(ids)

    marks = [2] + [PRE - 5 + (5 * (d - 1) + 1) // (E - 2) for d in range(1, E)]
    for d in range(1, E):
        turn_range(marks[d - 1], marks[d])
        if d == E - 1:
            pass_on(0)
            routing()
        landed = tok.at[0, rows_of(lax.rem(e + E - d, E)), :]
        arrived(landed, zt_send.at[d], zt_recv.at[d - 1])
        spread(landed, d)

    def early(first, last):
        for slot in range(first, last):
            fetched(slot)
        return range(first, last)

    def steps_of(p, n, ks, flip):
        def step(k, f):
            slot = k * pairs + p
            return (
                lambda: tok[k, :, f * TILE:(f + 1) * TILE],
                lambda: pool[slot, n * TILE:(n + 1) * TILE, f * TILE:(f + 1) * TILE] if flip else turned(slot, n, f),
                flip,
            )

        return [step(k, f) for k in ks for f in range(feats // TILE)]

    tiles = tall // TILE

    def sink_of(p, n, first, last):
        def sink(value):
            at = (p, slice(None), slice(n * TILE, (n + 1) * TILE))
            acc[at] = value if first else acc[at] + value
            if last and n == tiles - 1:
                finish(p)

        return sink

    def jobs_of(members, ks, first=False, last=False, flip=False):
        return [
            [
                (steps_of(p, n, ks, flip), sink_of(p, n, first, last))
                for p in members[q::2] for n in range(tiles)
            ]
            for q in range(2)
        ]

    def bands_of(slots):
        return [
            functools.partial(turn_piece, slot, r, f)
            for slot in slots for r in range(tall // LANES) for f in range(feats // TILE)
        ]

    low, high = list(range(half)), list(range(half, pairs))
    third, fourth = 2 * pairs, 3 * pairs

    def between():
        for d in range(E):
            from_side(1, d)
        pass_on(1)

    multiply(jobs_of(low, (0, 1), first=True), LAG, bands_of(early(PRE, third + half)), between, feats // TILE)
    fetch_down(T - 2)
    fetch_down(1)
    multiply(jobs_of(high, (0, 1), first=True), LAG, bands_of(early(third + half, fourth)))
    fetch_down(0)
    for d in range(2, E):
        pass_on(d)
    band = 32

    def finish_band(p, start):
        rows = slice(start, start + band)
        gate, up = acc[p, rows, :wide], acc[p, rows, wide:]
        weight = [
            jnp.sum(
                jnp.where(ids_t[rows] == e * experts + 2 * p + j, share_t[rows], 0.0), axis=1, keepdims=True
            )
            for j in range(2)
        ]
        first = lax.broadcasted_iota(jnp.int32, (band, wide), 1) < hidden_units
        value = gate / (1.0 + jnp.exp(-gate)) * up * jnp.where(first, weight[0], weight[1])
        hid[rows, p * wide:(p + 1) * wide] = value.astype(jnp.bfloat16)

    def finish(p):
        beside.extend(functools.partial(finish_band, p, start) for start in range(0, E * tok_rows, band))

    multiply(jobs_of(low + high, (2,)), LAG, bands_of(early(fourth, fourth + half)))
    for d in range(E):
        from_side(T - 1, d)
    late = high[half // 2:]
    some = early(fourth + half, fourth + half + half // 2)
    for p in late:
        fetched(fourth + p)
    plain, flipped = jobs_of(low, (3,), last=True), jobs_of(late, (3,), last=True, flip=True)
    multiply([plain[q] + flipped[q] for q in range(2)], LAG, bands_of(some), keep=True)
    parts_n = feats // TILE
    def down_ready(k):
        for q in range(half):
            fetched(down_slot[k] + q)

    def down_jobs(k, ns, sink_at, order=None):
        def step(n, m):
            start = m * TILE
            slot, f = down_slot[k] + m // tiles, m % tiles
            return (
                lambda: hid[:, start:start + TILE],
                lambda: pool[slot, f * TILE:(f + 1) * TILE, n * TILE:(n + 1) * TILE],
                False,
            )

        order = range(half * tiles) if order is None else order
        return [[([step(n + q, m) for m in order], sink_at(n + q)) for n in ns] for q in range(2)]

    def side_sink(dx):
        def sink_at(n):
            def sink(value):
                to_partner[dx, n] = value.astype(jnp.bfloat16)
                go(
                    to_partner.at[dx, n], from_partner.at[dx, n],
                    p_send.at[dx, n], p_recv.at[dx, n], (g, e, peer(1)),
                )

            return sink

        return sink_at

    def across_z(dx, met):
        edge[dx] = met
        for j in range(1, E):
            to_edge[dx, j] = edge[dx, rows_of(lax.rem(e + j, E)), :].astype(jnp.bfloat16)
            go(
                to_edge.at[dx, j], from_edge.at[dx, j],
                edge_send.at[dx, j], edge_recv.at[dx, j - 1], (g, lax.rem(e + j, E), t),
            )

    def gathered_edge(dx):
        total = edge[dx, rows_of(e), :]
        for d in range(1, E):
            arrived(from_edge.at[dx, d], edge_send.at[dx, d], edge_recv.at[dx, d - 1])
            total += from_edge[dx, d].astype(jnp.float32)
        return total

    def meet_sink(dx):
        def sink_at(n):
            def sink(value):
                arrived(from_partner.at[dx, n], p_send.at[dx, n], p_recv.at[dx, n])
                met = value + from_partner[dx, n].astype(jnp.float32)
                if n == parts_n - 1:
                    across_z(dx, met)
                    return
                if not dx:
                    own[n] = met
                    return
                back = (X - dx) % X
                for j in range(CUTS):
                    m = n * CUTS + j
                    to_x[dx, m] = met[:, j * CUT:(j + 1) * CUT].astype(jnp.bfloat16)
                    go(
                        to_x.at[dx, m], from_x.at[back, m],
                        x_send.at[dx, m], x_recv.at[back - 1, m], (g, e, peer(2 * dx)),
                    )

            return sink

        return sink_at

    open_pairs = range(min(high) * wide // TILE, (min(high) + half // 2) * wide // TILE)
    order = [m for m in range(half * tiles) if m not in open_pairs] + list(open_pairs)
    down_ready(T - 1)
    multiply(jobs_of(high[:half // 2], (3,), last=True), LAG, keep=True)
    multiply(
        down_jobs(T - 1, range(0, parts_n, 2), side_sink(X - 1), order), 0, cut=len(order) - len(open_pairs)
    )
    for dx in reversed(range(X)):
        if dx < X - 1:
            down_ready(2 * dx + 1)
            for n in reversed(range(0, parts_n, 2)):
                multiply(down_jobs(2 * dx + 1, [n], side_sink(dx)), 0)
        down_ready(2 * dx)
        for n in range(0, parts_n, 2) if dx else reversed(range(0, parts_n, 2)):
            multiply(down_jobs(2 * dx, [n], meet_sink(dx)), 0)
    inner = (parts_n - 1) * CUTS
    for m in range(inner):
        n, columns = m // CUTS, slice(m % CUTS * CUT, (m % CUTS + 1) * CUT)
        for other in range(1, X):
            arrived(from_x.at[other, m], x_send.at[other, m], x_recv.at[other - 1, m])
            own[n, :, columns] += from_x[other, m].astype(jnp.float32)
        for j in range(1, E):
            to_z[j, m] = own[n, rows_of(lax.rem(e + j, E)), columns].astype(jnp.bfloat16)
            go(to_z.at[j, m], from_z.at[j, m], z_send.at[j, m], z_recv.at[j - 1, m], (g, lax.rem(e + j, E), t))
        if m == inner - CUTS:
            to_far[...] = gathered_edge(1).astype(jnp.bfloat16)
            go(to_far, from_far, far_send, far_recv, (g, e, peer(2)))
    for m in range(inner):
        n, columns = m // CUTS, slice(m % CUTS * CUT, (m % CUTS + 1) * CUT)
        total = own[n, rows_of(e), columns]
        for d in range(1, E):
            arrived(from_z.at[d, m], z_send.at[d, m], z_recv.at[d - 1, m])
            total += from_z[d, m].astype(jnp.float32)
        out_ref[:, m * CUT:(m + 1) * CUT] = total.astype(out_ref.dtype)
        if m == inner - 2:
            total = gathered_edge(0)
            arrived(from_far, far_send, far_recv)
            total += from_far[...].astype(jnp.float32)
            out_ref[:, inner * CUT:] = total.astype(out_ref.dtype)
    for copy in sent:
        copy.wait_send()


def scratch_of(tok_rows, feats, experts, hidden_units, E, T, per_token):
    bf16, f32, X, N = jnp.bfloat16, jnp.float32, T // 2, E * tok_rows
    parts_n, cuts_n, tall = feats // TILE, feats // CUT, 4 * hidden_units
    slots = slots_of(experts, T)
    dma = pltpu.SemaphoreType.DMA
    return [
        ((slots, tall, feats), bf16),
        ((T, N, feats), bf16),
        ((E, per_token, tok_rows), jnp.int32),
        ((E, per_token, tok_rows), jnp.int32),
        ((experts // 2, N, tall), f32),
        ((N, experts * hidden_units), bf16),
        ((X, parts_n, N, TILE), bf16),
        ((X, parts_n, N, TILE), bf16),
        ((X, cuts_n - CUTS, N, CUT), bf16),
        ((X, cuts_n - CUTS, N, CUT), bf16),
        ((E, cuts_n - CUTS, tok_rows, CUT), bf16),
        ((E, cuts_n - CUTS, tok_rows, CUT), bf16),
        ((parts_n - 1, N, TILE), f32),
        ((N, per_token), jnp.int32),
        ((N, per_token), f32),
        ((X, N, TILE), f32),
        ((X, E, tok_rows, TILE), bf16),
        ((X, E, tok_rows, TILE), bf16),
        ((tok_rows, TILE), bf16),
        ((tok_rows, TILE), bf16),
    ], [
        dma((E - 1,)), dma((2, E - 1)), dma((T - 1, E)), dma((X, parts_n)), dma((X - 1, cuts_n - CUTS)), dma((E - 1, cuts_n - CUTS)),
        dma((X, E - 1)), dma,
    ]


def fits_fused(sizes):
    tok_rows, feats, experts, hidden_units, E, T, per_token = sizes
    if T != 4 or E != 4 or experts != 16 or E * tok_rows != 128 or feats % 512 or tok_rows % 16:
        return False
    if 2 * hidden_units % 128 or hidden_units % 16:
        return False
    buffers, _ = scratch_of(*sizes)
    size = 0
    for shape, kind in buffers:
        count = jnp.dtype(kind).itemsize
        for length in shape:
            count *= length
        size += count
    return size < VMEM_BYTES - 1_000_000


def on_device(tokens, expert_ids, gate_fixed, w_gate, w_up, w_down):
    (tok_rows, feats), per_token = tokens.shape, expert_ids.shape[1]
    experts, width, hidden_units = w_gate.shape
    E, T = lax.axis_size("expert"), lax.axis_size("tensor")
    sizes = (tok_rows, feats, experts, hidden_units, E, T, per_token)
    if not fits_fused(sizes):
        return slotted(tokens, expert_ids, gate_fixed, w_gate, w_up, w_down)
    buffers, semaphores = scratch_of(*sizes)
    vmem, anywhere = pl.BlockSpec(memory_space=pltpu.VMEM), pl.BlockSpec(memory_space=pl.ANY)
    return pl.pallas_call(
        functools.partial(fused_kernel, *sizes[:6]),
        out_shape=pltpu.VMEM(tokens.shape, tokens.dtype),
        in_specs=[anywhere] * 6,
        out_specs=vmem,
        scratch_shapes=[pltpu.VMEM(shape, kind) for shape, kind in buffers] + semaphores,
        compiler_params=pltpu.CompilerParams(
            collective_id=0, has_side_effects=True, vmem_limit_bytes=VMEM_BYTES,
        ),
    )(
        tokens,
        expert_ids.T,
        gate_fixed.T,
        jnp.swapaxes(w_gate, 1, 2),
        jnp.swapaxes(w_up, 1, 2),
        w_down.reshape(experts * hidden_units, width),
    )


def solution(mesh):
    placed = (
        P(("groups", "expert"), "tensor"),
        P(("groups", "expert"), None),
        P(("groups", "expert"), None),
        P("expert", None, "tensor"),
        P("expert", None, "tensor"),
        P("expert", "tensor", None),
    )
    return jax.shard_map(
        on_device,
        mesh=mesh,
        in_specs=placed,
        out_specs=P(("groups", "expert"), "tensor"),
        check_vma=False,
    )
```
